32 devices in a mesh: gx: 4 (over y, x), gy: 4 (over z), gz: 2 (over core).
Axes of the slice: x: 2, y: 2, z: 4, core: 2. Of those that a mesh axis runs over, the one named last changes fastest.
Arguments:
- a_blocks: float32 [1664, 7, 128, 128], P(('gx', 'gy', 'gz')), as said below
- block_cols: int32 [1664, 7], P(('gx', 'gy', 'gz')), may hold values from 0 to 363, as said below
- agg_ids: int32 [1664], P(('gx', 'gy', 'gz')), may hold values from 0 to 51, as said below
- agg_counts: int32 [32], P(('gx', 'gy', 'gz')), may hold values from 1 to 52, as said below
- p0_blocks: float32 [1664, 6, 128], P(('gx', 'gy', 'gz')), may hold values from -6 to 6
- start_vec: float32 [1664, 128], P(('gx', 'gy', 'gz'))
Outputs:
- p_blocks: float32 [1664, 7, 6, 128], P(('gx', 'gy', 'gz'))
- p_cols: int32 [1664, 7], P(('gx', 'gy', 'gz'))
- power_vec: float32 [1664, 128], P(('gx', 'gy', 'gz'))
The draws below stay inside these ranges and needn't reach their ends.
Inputs may be any that keep to these rules, and one draw needn't show every extreme that they name: `block_cols`: entry 0 of each block row names the row itself; every neighbour that an entry names exists. `agg_ids`: below the count of the row's own subdomain. `agg_counts`: some subdomain has 52 aggregates. `a_blocks`: block 0 of each block row has a positive diagonal.
All inputs are finite; a program needn't handle non-finite values.
Results may differ from the reference program's by a relative error of at most 0.0003.
Values sent between devices are 32-bit elements; how exact they have to be, the bound alone decides.
No kernel may reach another device: no remote copies, remote signals or barrier semaphores. Data moves between devices by JAX's collectives and lax.ppermute only.
A program may use at most 128 MiB of HBM per device.

```python
import jax
import jax.numpy as jnp
from jax import lax

B = 128
NS = 6
K = 7
BR = 52
ITERS = 8
BLOCKS = 1664
N_GX = 4
N_GY = 4
N_GZ = 2


def counts_helper(key):
    device_count = N_GX * N_GY * N_GZ
    per_device = jax.random.randint(jax.random.fold_in(key, 11), (device_count,), 1, BR + 1)
    chosen = jax.random.randint(jax.random.fold_in(key, 12), (), 0, device_count)
    return jnp.where(jnp.arange(device_count) == chosen, BR, per_device).astype(jnp.int32)


def draw_agg_counts(key, part):
    return counts_helper(key)


def draw_agg_ids(key, part):
    counted = jnp.repeat(counts_helper(key), BR)
    return jax.random.randint(jax.random.fold_in(key, 13), (BLOCKS,), 0, counted).astype(jnp.int32)


def draw_block_cols(key, part):
    blocks_all = jnp.arange(BLOCKS)
    device_index = blocks_all // BR
    own_row = blocks_all % BR
    coord_x = device_index // (N_GY * N_GZ)
    coord_y = device_index // N_GZ % N_GY
    coord_z = device_index % N_GZ
    exists = jnp.stack([coord_x > 0, coord_x < N_GX - 1, coord_y > 0, coord_y < N_GY - 1, coord_z > 0, coord_z < N_GZ - 1], axis=1)
    chosen = jax.random.randint(jax.random.fold_in(key, 21), (BLOCKS, 6), 0, 2)
    remote_row = jax.random.randint(jax.random.fold_in(key, 22), (BLOCKS, 6), 0, BR)
    local_row = jax.random.randint(jax.random.fold_in(key, 23), (BLOCKS, 6), 0, BR)
    direction = jnp.arange(6)[None, :]
    use_remote = (chosen == 1) & exists
    picked = jnp.where(use_remote, BR + direction * BR + remote_row, local_row)
    return jnp.concatenate([own_row[:, None], picked], axis=1).astype(jnp.int32)


def draw_a_blocks(key, part):
    device_index = (jnp.arange(BLOCKS) // BR).astype(jnp.float32)
    device_count = N_GX * N_GY * N_GZ
    strength = 0.3 + 1.2 * device_index / max(device_count - 1, 1)
    noise = jax.random.normal(jax.random.fold_in(key, 31), (BLOCKS, K, B, B), jnp.float32)
    diagonal = jax.random.uniform(jax.random.fold_in(key, 32), (BLOCKS, B), jnp.float32, 1.0, 2.0)
    identity = jnp.eye(B, dtype=jnp.float32)
    inner = noise[:, 0] * (0.4 / B ** 0.5) * (1.0 - identity) + identity * diagonal[:, :, None]
    outer = noise[:, 1:] * (strength[:, None, None, None] / (6.0 * B) ** 0.5)
    return jnp.concatenate([inner[:, None], outer], axis=1)


def draw_start_vec(key, part):
    device_index = (jnp.arange(BLOCKS) // BR).astype(jnp.float32)
    device_count = N_GX * N_GY * N_GZ
    ramp = device_index / max(device_count - 1, 1)
    values = jax.random.normal(jax.random.fold_in(key, 41), (BLOCKS, B), jnp.float32)
    return values * (1.0 + 2.0 * ramp)[:, None]


def block_levels(own_key, shape, shards, smallest, top_value):
    loudness, own = 1.0, jax.random.fold_in(own_key, 6)
    for dim, blocks in shards:
        heights = jnp.exp(jax.random.uniform(jax.random.fold_in(own, dim), (blocks,), jnp.float32, smallest / len(shards), top_value / len(shards)))
        loudness = loudness * jnp.repeat(heights, shape[dim] // blocks).reshape([-1 if axis == dim else 1 for axis in range(len(shape))])
    return loudness


def gaussian(rng, shape, deviation, bound, split=(), kind=jnp.bfloat16):
    values = jax.random.normal(rng, shape, jnp.float32) * deviation
    if len(split) > 0:
        values = block_levels(rng, shape, split, -0.22, 0.18) * values
    return jnp.clip(values, min=-bound, max=bound).astype(kind)


def setup_inputs(seed: int = 0) -> dict:
    keys = jax.random.split(jax.random.key(seed), 7)
    a_blocks = draw_a_blocks(jax.random.fold_in(keys[6], 71), 0)
    block_cols = draw_block_cols(jax.random.fold_in(keys[6], 71), 0)
    agg_ids = draw_agg_ids(jax.random.fold_in(keys[6], 71), 0)
    agg_counts = draw_agg_counts(jax.random.fold_in(keys[6], 71), 0)
    p0_blocks = gaussian(keys[4], (BLOCKS, NS, B), 1.0, 6.0, ((0, 32),), jnp.float32)
    start_vec = draw_start_vec(jax.random.fold_in(keys[6], 71), 0)
    return {"a_blocks": a_blocks, "block_cols": block_cols, "agg_ids": agg_ids, "agg_counts": agg_counts, "p0_blocks": p0_blocks, "start_vec": start_vec}


precise_mode = lax.Precision.HIGHEST

def global_rows(block_cols):
    device_count = N_GX * N_GY * N_GZ
    shaped = block_cols.reshape(device_count, BR, K)
    device_index = jnp.arange(device_count, dtype=jnp.int32)[:, None, None]
    strides = jnp.array([-N_GY * N_GZ, N_GY * N_GZ, -N_GZ, N_GZ, -1, 1], dtype=jnp.int32)
    beyond = shaped - BR
    direction = jnp.clip(beyond // BR, 0, 5)
    neighbour_row = beyond % BR
    remote = (device_index + strides[direction]) * BR + neighbour_row
    own_rows = device_index * BR + shaped
    return jnp.where(shaped < BR, own_rows, remote).reshape(device_count * BR, K).astype(jnp.int32)

def reference(a_blocks, block_cols, agg_ids, agg_counts, p0_blocks, start_vec):
    target = global_rows(block_cols)
    diag_values = jnp.diagonal(a_blocks[:, 0], axis1=1, axis2=2)

    def operate(vector):
        picked = vector[target]
        mixed = jnp.einsum('bkij,bkj->bi', a_blocks, picked, precision=precise_mode)
        return mixed / diag_values
    previous = start_vec
    current = start_vec
    for turn_index in range(ITERS):
        previous = current
        current = operate(current)
    last_norm = jnp.sqrt(jnp.sum(current * current))
    spectral = last_norm / jnp.sqrt(jnp.sum(previous * previous))
    power_vec = current * (jnp.sqrt(jnp.float32(BLOCKS * B)) / last_norm)
    damping = 4.0 / (3.0 * spectral)
    picked_p0 = p0_blocks[target]
    product = jnp.einsum('bksj,bkij->bksi', picked_p0, a_blocks, precision=precise_mode)
    smoothed = -(damping / diag_values)[:, None, None, :] * product
    p_blocks = smoothed.at[:, 0].add(p0_blocks)
    offsets = (jnp.cumsum(agg_counts) - agg_counts).astype(jnp.int32)
    p_cols = NS * (offsets[target // BR] + agg_ids[target])
    return (p_blocks, p_cols.astype(jnp.int32), power_vec)
```

```python
import jax
import jax.numpy as jnp
from jax import lax
from jax.experimental import pallas as pl
from jax.experimental.pallas import tpu as pltpu
from jax.sharding import PartitionSpec as P

ITERS = 8
AXES = ("gx", "gy", "gz")
MIB = 1 << 20
VMEM = pl.BlockSpec(memory_space=pltpu.VMEM)
SMEM = pl.BlockSpec(memory_space=pltpu.SMEM)
ANY = pl.BlockSpec(memory_space=pl.ANY)


def matchings(count):
    out = []
    for first in (0, 1):
        pairs = []
        for i in range(first, count - 1, 2):
            pairs += [(i, i + 1), (i + 1, i)]
        out.append(pairs)
    return out


def exchange(value):
    received, slots, used = [], [], 0
    for axis in AXES:
        mine = lax.axis_index(axis)
        base = used
        place = []
        for pairs in matchings(lax.axis_size(axis)):
            if pairs:
                received.append(lax.ppermute(value, axis, pairs))
                used += 1
            place.append(max(used, 1))
        even = (mine % 2) == 0
        slots.append(jnp.where(even, place[1], place[0]))
        slots.append(jnp.where(even, place[0], place[1]))
    return received, slots


def summed(value):
    for axis in reversed(AXES):
        count = lax.axis_size(axis)
        total = value
        for step in range(1, count):
            total = total + lax.ppermute(
                value, axis, [(i, (i + step) % count) for i in range(count)]
            )
        value = total
    return value


def split(value):
    high = value.astype(jnp.bfloat16)
    low = (value - high.astype(jnp.float32)).astype(jnp.bfloat16)
    return high, low


def dot_t(left, right):
    return lax.dot_general(
        left, right, (((1,), (1,)), ((), ())), preferred_element_type=jnp.float32
    )


def load_kernel(a_hbm, a_ref, sem):
    copy = pltpu.make_async_copy(a_hbm, a_ref, sem)
    copy.start()
    copy.wait()


def first_kernel(faces, index_ref, a_ref, *refs):
    own_ref, face_refs = refs[0], refs[1 : 1 + faces]
    prod_ref, z_ref, diag_ref, table = refs[1 + faces :]
    nb, nk, size, _ = a_ref.shape
    table[0:nb] = own_ref[...]
    for d in range(faces):
        table[(d + 1) * nb : (d + 2) * nb] = face_refs[d][...]
    sub = lax.broadcasted_iota(jnp.int32, (8, size), 0)

    def body(b, _):
        total = jnp.zeros((8, size), jnp.float32)
        for k in range(nk):
            block = a_ref[b, k]
            if k == 0:
                eye = lax.broadcasted_iota(jnp.int32, (size, size), 0) == (
                    lax.broadcasted_iota(jnp.int32, (size, size), 1)
                )
                diag = jnp.sum(jnp.where(eye, block, 0.0), axis=0, keepdims=True)
                diag_ref[pl.ds(b, 1), :] = diag
            rows = table[index_ref[b * nk + k]]
            rows_high, rows_low = split(rows)
            high, low = split(block)
            product = dot_t(rows_high, high) + (dot_t(rows_low, high) + dot_t(rows_high, low))
            total = total + product
            prod_ref[b * nk + k] = jnp.where(sub == 7, rows, product)
        z_ref[pl.ds(b, 1), :] = total[0:1, :] / diag
        return 0

    lax.fori_loop(0, nb, body, 0)


def step_kernel(faces, last, index_ref, a_ref, *refs):
    own_ref, face_refs = refs[0], refs[1 : 1 + faces]
    diag_ref = refs[1 + faces]
    outs = refs[2 + faces :]
    z_ref, table = outs[0], outs[-1]
    nb, nk, size, _ = a_ref.shape
    stride = table.shape[0] // (faces + 1)
    table[0:nb, :] = own_ref[...]
    for d in range(faces):
        table[(d + 1) * stride : (d + 1) * stride + nb, :] = face_refs[d][...]
    ones = jnp.ones((8, size), jnp.bfloat16)

    def body(b, _):
        acc = None
        for k in range(nk):
            term = a_ref[b, k] * table[pl.ds(index_ref[b * nk + k], 1), :]
            acc = term if acc is None else acc + term
        high, low = split(acc)
        row = dot_t(ones, high) + dot_t(ones, low)
        z_ref[pl.ds(b, 1), :] = row[0:1, :] / diag_ref[pl.ds(b, 1), :]
        return 0

    lax.fori_loop(0, nb, body, 0, unroll=2 if nb % 2 == 0 else 1)
    if last:
        before, now = own_ref[...], z_ref[...]
        outs[1][0:1, :] = jnp.sum(before * before, axis=0, keepdims=True)
        outs[1][1:2, :] = jnp.sum(now * now, axis=0, keepdims=True)


def final_kernel(root_total, ids_ref, totals_ref, cols_ref, prod_ref, x_ref, diag_ref, z_ref, *outs):
    p_ref, c_ref, power_ref = outs
    nk, ns, nb, size = p_ref.shape
    totals = totals_ref[...]
    last_norm = jnp.sqrt(totals[:, 1:2])
    spectral = last_norm / jnp.sqrt(totals[:, 0:1])
    damping = 4.0 / (3.0 * spectral)
    power_ref[...] = z_ref[...] * (root_total / last_norm)
    lane = lax.broadcasted_iota(jnp.int32, totals.shape, 1) - 2
    offsets = [
        jnp.sum(
            jnp.where((lane >= 0) & (lane < ids_ref[d]), totals, 0.0), axis=1, keepdims=True
        )
        for d in range(7)
    ]
    for start in range(0, nb, 8):
        n = min(8, nb - start)
        scale = damping / diag_ref[start : start + n, :]
        cols = cols_ref[start : start + n, :]
        base = jnp.broadcast_to(offsets[0], cols.shape)
        for d in range(1, 7):
            base = jnp.where(cols >= d * nb, offsets[d], base)
        column = lax.broadcasted_iota(jnp.int32, cols.shape, 1)
        for k in range(nk):
            at = (start * nk + k) * 8
            for s in range(ns):
                value = -scale * prod_ref[pl.ds(at + s + 1, n, stride=nk * 8), :]
                if k == 0:
                    value = value + x_ref[pl.ds(start * 8 + s + 1, n, stride=8), :]
                p_ref[k, s, start : start + n, :] = value
            names = prod_ref[pl.ds(at + 7, n, stride=nk * 8), :]
            base = base + jnp.where(column == k, names[:, : cols.shape[1]], 0.0)
        c_ref[start : start + n, :] = ns * base.astype(jnp.int32)


def call(kernel, out_shape, in_specs, scratch=(), limit=34 * MIB):
    many = isinstance(out_shape, (tuple, list))
    return pl.pallas_call(
        kernel,
        out_shape=out_shape,
        in_specs=in_specs,
        out_specs=tuple(VMEM for _ in out_shape) if many else VMEM,
        scratch_shapes=list(scratch),
        compiler_params=pltpu.CompilerParams(vmem_limit_bytes=limit),
    )


def local(a_blocks, block_cols, agg_ids, agg_counts, p0_blocks, start_vec):
    nb, nk, size, _ = a_blocks.shape
    ns = p0_blocks.shape[1]
    f32 = jnp.float32
    devices = 1
    me = jnp.int32(0)
    for axis in AXES:
        devices *= lax.axis_size(axis)
        me = me * lax.axis_size(axis) + lax.axis_index(axis)
    strides = (lax.axis_size("gy") * lax.axis_size("gz"), lax.axis_size("gz"), 1)
    ids = jnp.stack([me] + [me + sign * s for s in strides for sign in (-1, 1)])

    a_here = call(
        load_kernel,
        pltpu.VMEM(a_blocks.shape, f32),
        [ANY],
        [pltpu.SemaphoreType.DMA],
    )(a_blocks)

    names = jnp.broadcast_to(agg_ids.astype(f32)[:, None, None], (nb, 1, size))
    x_own = jnp.concatenate([start_vec[:, None, :], p0_blocks, names], axis=1)
    x_faces, slots = exchange(x_own)
    faces = len(x_faces)
    way = block_cols // nb
    slot = jnp.zeros_like(block_cols)
    for d in range(6):
        slot = jnp.where(way == d + 1, slots[d], slot)
    row = block_cols - way * nb
    stride = -(-nb // 8) * 8
    first_index = (slot * nb + row).reshape(-1)
    index = (slot * stride + row).reshape(-1)

    prod, current, diag = call(
        lambda *r: first_kernel(faces, *r),
        (
            jax.ShapeDtypeStruct((nb * nk, 8, size), f32),
            jax.ShapeDtypeStruct((nb, size), f32),
            jax.ShapeDtypeStruct((nb, size), f32),
        ),
        [SMEM, VMEM, VMEM] + [VMEM] * faces,
        [pltpu.VMEM(((faces + 1) * nb, 8, size), f32)],
    )(first_index, a_here, x_own, *x_faces)

    for turn in range(1, ITERS):
        last = turn == ITERS - 1
        received, _ = exchange(current)
        shapes = [jax.ShapeDtypeStruct((nb, size), f32)]
        if last:
            shapes.append(jax.ShapeDtypeStruct((2, size), f32))
        results = call(
            lambda *r, last=last: step_kernel(faces, last, *r),
            tuple(shapes),
            [SMEM, VMEM, VMEM] + [VMEM] * faces + [VMEM],
            [pltpu.VMEM(((faces + 1) * stride, size), f32)],
        )(index, a_here, current, *received, diag)
        current = results[0]

    mark = jnp.where(jnp.arange(devices) == me, agg_counts[0].astype(f32), 0.0)
    totals = summed(jnp.concatenate([jnp.sum(results[1], axis=1), mark])[None, :])

    smoothed, p_cols, power_vec = call(
        lambda *r: final_kernel(float((devices * nb * size) ** 0.5), *r),
        (
            jax.ShapeDtypeStruct((nk, ns, nb, size), f32),
            jax.ShapeDtypeStruct((nb, nk), jnp.int32),
            jax.ShapeDtypeStruct((nb, size), f32),
        ),
        [SMEM] + [VMEM] * 6,
    )(
        ids,
        totals,
        block_cols,
        prod.reshape(nb * nk * 8, size),
        x_own.reshape(nb * 8, size),
        diag,
        current,
    )
    return jnp.transpose(smoothed, (2, 0, 1, 3)), p_cols, power_vec


def solution(mesh):
    spec = P(AXES)
    return jax.shard_map(
        local, mesh=mesh, in_specs=(spec,) * 6, out_specs=(spec,) * 3, check_vma=False
    )
```

```python
import jax
import jax.numpy as jnp
from jax import lax
from jax.experimental import pallas as pl
from jax.experimental.pallas import tpu as pltpu
from jax.sharding import PartitionSpec as P

ITERS = 8
AXES = ("gx", "gy", "gz")
MIB = 1 << 20
VMEM = pl.BlockSpec(memory_space=pltpu.VMEM)
SMEM = pl.BlockSpec(memory_space=pltpu.SMEM)
ANY = pl.BlockSpec(memory_space=pl.ANY)


def matchings(count):
    out = []
    for first in (0, 1):
        pairs = []
        for i in range(first, count - 1, 2):
            pairs += [(i, i + 1), (i + 1, i)]
        out.append(pairs)
    return out


def exchange(value):
    received, slots, used = [], [], 0
    for axis in AXES:
        mine = lax.axis_index(axis)
        place = []
        for pairs in matchings(lax.axis_size(axis)):
            if pairs:
                received.append(lax.ppermute(value, axis, pairs))
                used += 1
            place.append(max(used, 1))
        even = (mine % 2) == 0
        slots.append(jnp.where(even, place[1], place[0]))
        slots.append(jnp.where(even, place[0], place[1]))
    return received, slots


def summed(value):
    for axis in reversed(AXES):
        count = lax.axis_size(axis)
        total = value
        for step in range(1, count):
            total = total + lax.ppermute(
                value, axis, [(i, (i + step) % count) for i in range(count)]
            )
        value = total
    return value


def split(value):
    high = value.astype(jnp.bfloat16)
    low = (value - high.astype(jnp.float32)).astype(jnp.bfloat16)
    return high, low


def dot_t(left, right):
    return lax.dot_general(
        left, right, (((1,), (1,)), ((), ())), preferred_element_type=jnp.float32
    )


def group_of(count):
    return next(g for g in (4, 3, 2, 1) if count % g == 0)


def first_kernel(faces, index_ref, a_hbm, *refs):
    own_ref, face_refs = refs[0], refs[1 : 1 + faces]
    prod_ref, z_ref, diag_ref, a_ref, table, sems = refs[-6:]
    nb, nk, size, _ = a_ref.shape
    group = group_of(nb)

    def piece(g):
        part = pl.ds(g * group, group)
        return pltpu.make_async_copy(a_hbm.at[part], a_ref.at[part], sems.at[g])

    for g in range(nb // group):
        piece(g).start()
    table[0:nb] = own_ref[...]
    for d in range(faces):
        table[(d + 1) * nb : (d + 2) * nb] = face_refs[d][...]
    sub = lax.broadcasted_iota(jnp.int32, (8, size), 0)
    eye = lax.broadcasted_iota(jnp.int32, (size, size), 0) == (
        lax.broadcasted_iota(jnp.int32, (size, size), 1)
    )

    def body(g, _):
        piece(g).wait()
        for u in range(group):
            b = g * group + u
            diag = jnp.sum(jnp.where(eye, a_ref[b, 0], 0.0), axis=0, keepdims=True)
            diag_ref[pl.ds(b, 1), :] = diag
            total = jnp.zeros((8, size), jnp.float32)
            for k in range(nk):
                rows = table[index_ref[b * nk + k]]
                rows_high, rows_low = split(rows)
                high, low = split(a_ref[b, k])
                both = dot_t(jnp.concatenate([rows_high, rows_low], axis=0), high)
                product = both[0:8] + (both[8:16] + dot_t(rows_high, low))
                total = total + product
                prod_ref[b * nk + k] = jnp.where(sub == 7, rows, product)
            z_ref[pl.ds(b, 1), :] = total[0:1, :] / diag
        return 0

    lax.fori_loop(0, nb // group, body, 0)


def step_kernel(faces, last, index_ref, a_ref, *refs):
    own_ref, face_refs = refs[0], refs[1 : 1 + faces]
    diag_ref = refs[1 + faces]
    outs = refs[2 + faces :]
    z_ref, table = outs[0], outs[-1]
    nb, nk, size, _ = a_ref.shape
    stride = table.shape[0] // (faces + 1)
    table[0:nb, :] = own_ref[...]
    for d in range(faces):
        table[(d + 1) * stride : (d + 1) * stride + nb, :] = face_refs[d][...]
    width = -(-nb // size) * size
    lane = lax.broadcasted_iota(jnp.int32, (size, width), 1)
    group = group_of(nb)

    def body(g, columns):
        for u in range(group):
            b = g * group + u
            acc = None
            for k in range(nk):
                term = a_ref[b, k] * table[pl.ds(index_ref[b * nk + k], 1), :]
                acc = term if acc is None else acc + term
            columns = jnp.where(lane == b, jnp.sum(acc, axis=1, keepdims=True), columns)
        return columns

    columns = lax.fori_loop(0, nb // group, body, jnp.zeros((size, width), jnp.float32))
    z_ref[...] = columns.T[0:nb, :] / diag_ref[...]
    if last:
        before, now = own_ref[...], z_ref[...]
        outs[1][0:1, :] = jnp.sum(before * before, axis=0, keepdims=True)
        outs[1][1:2, :] = jnp.sum(now * now, axis=0, keepdims=True)


def final_kernel(root_total, ids_ref, totals_ref, cols_ref, prod_ref, x_ref, diag_ref, z_ref, *outs):
    p_ref, c_ref, power_ref = outs
    nk, ns, nb, size = p_ref.shape
    totals = totals_ref[...]
    last_norm = jnp.sqrt(totals[:, 1:2])
    spectral = last_norm / jnp.sqrt(totals[:, 0:1])
    damping = 4.0 / (3.0 * spectral)
    power_ref[...] = z_ref[...] * (root_total / last_norm)
    lane = lax.broadcasted_iota(jnp.int32, totals.shape, 1) - 2
    offsets = [
        jnp.sum(
            jnp.where((lane >= 0) & (lane < ids_ref[d]), totals, 0.0), axis=1, keepdims=True
        )
        for d in range(7)
    ]
    for start in range(0, nb, 8):
        n = min(8, nb - start)
        scale = damping / diag_ref[start : start + n, :]
        cols = cols_ref[start : start + n, :]
        base = jnp.broadcast_to(offsets[0], cols.shape)
        for d in range(1, 7):
            base = jnp.where(cols >= d * nb, offsets[d], base)
        column = lax.broadcasted_iota(jnp.int32, cols.shape, 1)
        for k in range(nk):
            at = (start * nk + k) * 8
            for s in range(ns):
                value = -scale * prod_ref[pl.ds(at + s + 1, n, stride=nk * 8), :]
                if k == 0:
                    value = value + x_ref[pl.ds(start * 8 + s + 1, n, stride=8), :]
                p_ref[k, s, start : start + n, :] = value
            names = prod_ref[pl.ds(at + 7, n, stride=nk * 8), :]
            base = base + jnp.where(column == k, names[:, : cols.shape[1]], 0.0)
        c_ref[start : start + n, :] = ns * base.astype(jnp.int32)


def call(kernel, out_shape, in_specs, scratch=(), limit=8 * MIB):
    many = isinstance(out_shape, (tuple, list))
    return pl.pallas_call(
        kernel,
        out_shape=out_shape,
        in_specs=in_specs,
        out_specs=tuple(VMEM for _ in out_shape) if many else VMEM,
        scratch_shapes=list(scratch),
        compiler_params=pltpu.CompilerParams(vmem_limit_bytes=limit),
    )


def local(a_blocks, block_cols, agg_ids, agg_counts, p0_blocks, start_vec):
    nb, nk, size, _ = a_blocks.shape
    ns = p0_blocks.shape[1]
    f32 = jnp.float32
    devices = 1
    me = jnp.int32(0)
    for axis in AXES:
        devices *= lax.axis_size(axis)
        me = me * lax.axis_size(axis) + lax.axis_index(axis)
    strides = (lax.axis_size("gy") * lax.axis_size("gz"), lax.axis_size("gz"), 1)
    ids = jnp.stack([me] + [me + sign * s for s in strides for sign in (-1, 1)])

    names = jnp.broadcast_to(agg_ids.astype(f32)[:, None, None], (nb, 1, size))
    x_own = jnp.concatenate([start_vec[:, None, :], p0_blocks, names], axis=1)
    x_faces, slots = exchange(x_own)
    faces = len(x_faces)
    way = block_cols // nb
    slot = jnp.zeros_like(block_cols)
    for d in range(6):
        slot = jnp.where(way == d + 1, slots[d], slot)
    row = block_cols - way * nb
    stride = -(-nb // 8) * 8
    first_index = (slot * nb + row).reshape(-1)
    index = (slot * stride + row).reshape(-1)

    mark = jnp.where(jnp.arange(devices) == me, agg_counts[0].astype(f32), 0.0)
    x_flat = x_own.reshape(nb * 8, size)
    early = (index, ids, block_cols, mark, x_flat)

    prod, current, diag, a_here = call(
        lambda *r: first_kernel(faces, *r),
        (
            jax.ShapeDtypeStruct((nb * nk, 8, size), f32),
            jax.ShapeDtypeStruct((nb, size), f32),
            jax.ShapeDtypeStruct((nb, size), f32),
            pltpu.VMEM(a_blocks.shape, f32),
        ),
        [SMEM, ANY, VMEM] + [VMEM] * faces + [ANY] * len(early),
        [
            pltpu.VMEM(((faces + 1) * nb, 8, size), f32),
            pltpu.SemaphoreType.DMA((nb // group_of(nb),)),
        ],
    )(first_index, a_blocks, x_own, *x_faces, *early)

    for turn in range(1, ITERS):
        last = turn == ITERS - 1
        received, _ = exchange(current)
        shapes = [jax.ShapeDtypeStruct((nb, size), f32)]
        if last:
            shapes.append(jax.ShapeDtypeStruct((2, size), f32))
        results = call(
            lambda *r, last=last: step_kernel(faces, last, *r),
            tuple(shapes),
            [SMEM, VMEM, VMEM] + [VMEM] * faces + [VMEM],
            [pltpu.VMEM(((faces + 1) * stride, size), f32)],
        )(index, a_here, current, *received, diag)
        current = results[0]

    totals = summed(jnp.concatenate([jnp.sum(results[1], axis=1), mark])[None, :])

    smoothed, p_cols, power_vec = call(
        lambda *r: final_kernel(float((devices * nb * size) ** 0.5), *r),
        (
            jax.ShapeDtypeStruct((nk, ns, nb, size), f32),
            jax.ShapeDtypeStruct((nb, nk), jnp.int32),
            jax.ShapeDtypeStruct((nb, size), f32),
        ),
        [SMEM] + [VMEM] * 6,
    )(
        ids,
        totals,
        block_cols,
        prod.reshape(nb * nk * 8, size),
        x_flat,
        diag,
        current,
    )
    return jnp.transpose(smoothed, (2, 0, 1, 3)), p_cols, power_vec


def solution(mesh):
    spec = P(AXES)
    return jax.shard_map(
        local, mesh=mesh, in_specs=(spec,) * 6, out_specs=(spec,) * 3, check_vma=False
    )
```
